32 devices in a mesh: gx: 8 (over y, x, core), gy: 4 (over z).
Axes of the slice: x: 2, y: 2, z: 4, core: 2. Of those that a mesh axis runs over, the one named last changes fastest.
Arguments:
- density: float32 [32, 256, 256], P(('gx', 'gy')), may hold values from -0.06 to 0.56, as said below
- coupling: float32 [32, 256, 256], P(('gx', 'gy')), may hold values from -0.04 to 0.04
- weights: float32 [32], P(('gx', 'gy')), may hold values from 0.25 to 2
- live_mask: int32 [32], P(('gx', 'gy')), may hold values 0 or 1
- dimer_pairs: int32 [32, 2], replicated, may hold values from 0 to 31, as said below
- dimer_slot: int32 [32], replicated, may hold values from 0 to 31, as said below
- frag_slot: int32 [32], replicated, may hold values from 0 to 31, as said below
Outputs:
- refined: float32 [32, 256, 256], P(('gx', 'gy'))
The draws below stay inside these ranges and needn't reach their ends.
Inputs may be any that keep to these rules, and one draw needn't show every extreme that they name: `dimer_slot`: each slot holds exactly one listed dimer. `frag_slot`: each fragment has its own slot; slot q lies on device q, devices numbered with gy fastest. `dimer_pairs`: the two fragments of a dimer differ. The dimers in slots k * 1 to (k + 1) - 1 (device k) name 2 fragments whose storage devices have pairwise different gx indices and pairwise different gy indices. `density`: each block is symmetric.
All inputs are finite; a program needn't handle non-finite values. No bound on the sum of `live_mask` on one device may be relied on, other than what follows from the above.
Results may differ from the reference program's by a relative error of at most 0.0003.
Values sent between devices are 32-bit elements; how exact they have to be, the bound alone decides.
A program may use at most 64 MiB of HBM per device.

```python
import math
import jax
import jax.numpy as jnp
from jax import lax

B = 256
FRAG_DEV = 1
ITERS = 3
SWEEPS = 1
DIM_DEV = 1
FRAGMENTS = 32
DIMERS = 32
N_GX = 8
N_GY = 4


def routing_plan(key):
    frag_key = jax.random.fold_in(key, 101)
    dimer_key = jax.random.fold_in(key, 202)
    row_key = jax.random.fold_in(key, 303)
    column_key = jax.random.fold_in(key, 404)
    local_key = jax.random.fold_in(key, 505)
    frag_slot = jax.random.permutation(frag_key, FRAGMENTS).astype(jnp.int32)
    dimer_slot = jax.random.permutation(dimer_key, DIMERS).astype(jnp.int32)
    devices_all = N_GX * N_GY
    refs = 2 * DIM_DEV
    row_keys = jax.random.split(row_key, devices_all)
    column_keys = jax.random.split(column_key, devices_all)
    pick_x = jax.vmap(lambda one_key: jax.random.permutation(one_key, N_GX)[:refs])(row_keys)
    pick_y = jax.vmap(lambda one_key: jax.random.permutation(one_key, N_GY)[:refs])(column_keys)
    local_part = jax.random.randint(local_key, (devices_all, refs), 0, FRAG_DEV)
    ref_slot = ((pick_x * N_GY + pick_y) * FRAG_DEV + local_part).astype(jnp.int32).reshape(DIMERS, 2)
    inverse = jnp.argsort(frag_slot).astype(jnp.int32)
    slot_frags = inverse[ref_slot]
    dimer_pairs = slot_frags[dimer_slot]
    return (dimer_pairs.astype(jnp.int32), dimer_slot, frag_slot)


def draw_dimer_pairs(key, part):
    return routing_plan(key)[0]


def draw_dimer_slot(key, part):
    return routing_plan(key)[1]


def draw_frag_slot(key, part):
    return routing_plan(key)[2]


def draw_density(key, part):
    noise_key = jax.random.fold_in(key, 606)
    raw = jnp.clip(jax.random.normal(noise_key, (FRAGMENTS, B, B), jnp.float32), -4.0, 4.0)
    symmetric = (raw + jnp.swapaxes(raw, 1, 2)) * (0.01 / 1.4142135)
    return symmetric + 0.5 * jnp.eye(B, dtype=jnp.float32)[None, :, :]


def draw_coupling(key, part):
    noise_key = jax.random.fold_in(key, 707)
    raw = jnp.clip(jax.random.normal(noise_key, (DIMERS, B, B), jnp.float32), -4.0, 4.0)
    return raw * 0.01


def place_ends(drawn, key, low, largest):
    index_at = [jax.random.randint(jax.random.fold_in(key, axis), (), 0, length) for axis, length in enumerate(drawn.shape)]
    main_axis = drawn.shape.index(max(drawn.shape))
    beside = index_at[:main_axis] + [(index_at[main_axis] + 1) % drawn.shape[main_axis]] + index_at[main_axis + 1:]
    return drawn.at[tuple(index_at)].set(low).at[tuple(beside)].set(largest)


def shard_levels(rng, extent, cuts, least, high):
    factor_of, own = 1.0, jax.random.fold_in(rng, 6)
    for position, parts in cuts:
        steps = jnp.exp(jax.random.uniform(jax.random.fold_in(own, position), (parts,), jnp.float32, least / len(cuts), high / len(cuts)))
        factor_of = factor_of * jnp.repeat(steps, extent[position] // parts).reshape([-1 if axis == position else 1 for axis in range(len(extent))])
    return factor_of


def setup_inputs(seed: int = 0) -> dict:
    splits = jax.random.split(jax.random.key(seed), 8)
    density = draw_density(jax.random.fold_in(splits[7], 71), 0)
    coupling = draw_coupling(jax.random.fold_in(splits[7], 71), 0)
    weights = jnp.clip(jnp.exp(math.log(2.0) - 2.0794415 * jax.random.uniform(splits[2], (DIMERS,), jnp.float32) ** shard_levels(splits[2], (DIMERS,), ((0, 32),), -0.2, 0.2)), 0.25, 2.0)
    live_mask = place_ends((jax.random.randint(splits[3], (DIMERS,), 0, 4) < 3).astype(jnp.int32), jax.random.fold_in(splits[3], 1), 0, 1)
    dimer_pairs = draw_dimer_pairs(jax.random.fold_in(splits[7], 71), 0)
    dimer_slot = draw_dimer_slot(jax.random.fold_in(splits[7], 71), 0)
    frag_slot = draw_frag_slot(jax.random.fold_in(splits[7], 71), 0)
    return dict(density=density, coupling=coupling, weights=weights, live_mask=live_mask, dimer_pairs=dimer_pairs, dimer_slot=dimer_slot, frag_slot=frag_slot)


def product(left, right):
    return jnp.dot(left, right, precision=lax.Precision.HIGHEST, preferred_element_type=jnp.float32)


def purify(first_block, second_block, coupling_block):
    half_width = first_block.shape[0]
    upper_rows = jnp.concatenate([first_block, coupling_block], axis=1)
    lower_rows = jnp.concatenate([coupling_block.T, second_block], axis=1)
    matrix = jnp.concatenate([upper_rows, lower_rows], axis=0)
    for repeat in range(ITERS):
        square = product(matrix, matrix)
        matrix = 3.0 * square - 2.0 * product(square, matrix)
    return matrix[:half_width, :half_width], matrix[half_width:, half_width:]


def reference(density, coupling, weights, live_mask, dimer_pairs, dimer_slot, frag_slot):
    blocks = density
    for sweep_index in range(SWEEPS):
        def visit(carry, dimer_index):
            totals, weight_sums = carry
            slot_index = dimer_slot[dimer_index]
            first_slot = frag_slot[dimer_pairs[dimer_index, 0]]
            second_slot = frag_slot[dimer_pairs[dimer_index, 1]]
            factor = jnp.where(live_mask[slot_index] > 0, weights[slot_index], jnp.float32(0.0))
            first_new, second_new = purify(blocks[first_slot], blocks[second_slot], coupling[slot_index])
            totals = totals.at[first_slot].add(factor * first_new)
            totals = totals.at[second_slot].add(factor * second_new)
            weight_sums = weight_sums.at[first_slot].add(factor)
            weight_sums = weight_sums.at[second_slot].add(factor)
            return (totals, weight_sums), dimer_index

        start = (jnp.zeros(blocks.shape, jnp.float32), jnp.zeros((blocks.shape[0],), jnp.float32))
        finals, ignored = lax.scan(visit, start, jnp.arange(dimer_pairs.shape[0], dtype=jnp.int32))
        totals, weight_sums = finals
        blocks = (blocks + totals) / (1.0 + weight_sums)[:, None, None]
    return blocks
```

```python
import functools
import jax
import jax.numpy as jnp
from jax import lax
from jax.experimental import pallas as pl
from jax.experimental.pallas import tpu as pltpu
from jax.sharding import PartitionSpec as P

ITERS = 3
MESH = pl.DeviceIdType.MESH
F32 = jnp.float32
BF16 = jnp.bfloat16


def split(value):
    high = value.astype(BF16)
    return high, (value - high.astype(F32)).astype(BF16)


def mm(left, right):
    return jnp.dot(left, right, preferred_element_type=F32)


def wrap(index, count):
    return jnp.where(index < 0, index + count, index)


def grid_iota(rows, columns):
    return (
        lax.broadcasted_iota(jnp.int32, (rows, columns), 0),
        lax.broadcasted_iota(jnp.int32, (rows, columns), 1),
    )


def kernel(
    count_x, count_y,
    density_ref, coupling_ref, weights_ref, live_ref, pairs_ref, dslot_ref, fslot_ref,
    out_ref,
    codes, refs_s, packed, held, diag, held_diag, chosen, got, joined,
    matrix, m_high, m_low, q_high, q_low, square,
    grown, landed, extra, landed_extra, flat, table, totals, back,
    send_sems, recv_sems,
):
    count = count_x * count_y
    dim_dev = coupling_ref.shape[0]
    refs = 2 * dim_dev
    dimers = dslot_ref.shape[0]
    width = density_ref.shape[1]
    half = width // 2
    rows = width // count
    me = lax.axis_index("gx") * count_y + lax.axis_index("gy")

    def peer(step):
        other = lax.rem(me + step, count)
        return other, (lax.div(other, count_y), lax.rem(other, count_y))

    barrier = pltpu.get_barrier_semaphore()

    def greet(step, carry):
        pl.semaphore_signal(barrier, inc=1, device_id=peer(step)[1], device_id_type=MESH)
        return carry

    lax.fori_loop(1, count, greet, 0)

    row_id, column_id = grid_iota(half, half)
    upper = row_id <= column_id
    strict = row_id > column_id
    on_diag = row_id == column_id

    def pack(first, corner, second):
        mixed = jnp.where(upper, first, second)
        return corner, mixed, jnp.sum(jnp.where(on_diag, second, 0.0), axis=0, keepdims=True)

    def scatter_rows(target, corner, mixed):
        for piece in range(count):
            start = piece * rows
            source = corner if start < half else mixed
            start = start % half
            target(piece, source[start:start + rows])

    corner, mixed, diag_row = pack(
        density_ref[0, :half, :half], density_ref[0, :half, half:], density_ref[0, half:, half:]
    )

    def put_packed(piece, value):
        packed[piece] = value

    scatter_rows(put_packed, corner, mixed)
    diag[...] = diag_row

    pl.semaphore_wait(barrier, count - 1)

    def exchange(phase, source, target, same):
        def send(step, carry):
            other, where_to = peer(step)
            pltpu.make_async_remote_copy(
                src_ref=source if same else source.at[other],
                dst_ref=target.at[count - step],
                send_sem=send_sems.at[phase],
                recv_sem=recv_sems.at[phase],
                device_id=where_to,
                device_id_type=MESH,
            ).start()
            return carry

        lax.fori_loop(1, count, send, 0)

    def wait_for(sems, phase, target):
        span = target.at[pl.ds(1, count - 1)]
        pltpu.make_async_copy(span, span, sems.at[phase]).wait()

    exchange(0, packed, held, False)
    exchange(1, diag, held_diag, True)
    held[0] = packed[me]
    held_diag[0] = diag[...]

    def code_of(dimer, carry):
        codes[dimer] = fslot_ref[pairs_ref[dimer, 0]] * count + fslot_ref[pairs_ref[dimer, 1]]
        return carry

    lax.fori_loop(0, dimers, code_of, 0)

    def names(slot, carry):
        def look(dimer, found):
            return jnp.where(dslot_ref[dimer] == slot, codes[dimer], found)

        found = lax.fori_loop(0, dimers, look, jnp.int32(0), unroll=dimers <= 64)
        refs_s[2 * slot] = lax.div(found, jnp.int32(count))
        refs_s[2 * slot + 1] = lax.rem(found, jnp.int32(count))
        return carry

    lax.fori_loop(0, count * dim_dev, names, 0)

    wait_for(recv_sems, 0, held)

    def choose(target, carry):
        for ref in range(refs):
            slot = refs_s[target * refs + ref]
            chosen[target, ref] = held[wrap(slot - me, count)]
        return carry

    lax.fori_loop(0, count, choose, 0, unroll=count <= 32)
    exchange(2, chosen, got, False)
    got[0] = chosen[me]
    wait_for(recv_sems, 1, held_diag)

    lanes = count * refs * rows
    lane_id = lax.broadcasted_iota(jnp.int32, (1, lanes), 1)
    lane_ref = lane_id // rows

    def spread(entry, row):
        ref = lax.rem(entry, refs)
        source = lax.rem(me + lax.div(entry, refs), count)
        return jnp.where(lane_ref == entry, refs_s[source * refs + ref], row)

    named = lax.fori_loop(
        0, count * refs, spread, jnp.zeros((1, lanes), jnp.int32), unroll=count * refs <= 64
    )
    named = named * rows + lane_id % rows
    table_row = lax.broadcasted_iota(jnp.int32, (count * rows, lanes), 0)
    table[...] = jnp.where(table_row == named, 1.0, 0.0).astype(BF16)

    wait_for(recv_sems, 2, got)

    for dimer in range(dim_dev):
        coupled = coupling_ref[dimer]
        matrix[:width, width:] = coupled
        matrix[width:, :width] = coupled.T
        for side in range(2):
            ref = 2 * dimer + side
            for piece in range(count):
                joined[piece * rows:(piece + 1) * rows, :] = got[wrap(piece - me, count), ref]
            corner = joined[:half, :]
            mixed = joined[half:, :]
            turned = mixed.T
            slot = refs_s[me * refs + ref]
            diag_row = held_diag[wrap(slot - me, count)]
            low = side * width
            mid = low + half
            high = low + width
            matrix[low:mid, low:mid] = jnp.where(upper, mixed, turned)
            matrix[low:mid, mid:high] = corner
            matrix[mid:high, low:mid] = corner.T
            matrix[mid:high, mid:high] = jnp.where(
                on_diag, diag_row, jnp.where(strict, mixed, turned)
            )
        for repeat in range(ITERS):
            m_high[...], m_low[...] = split(matrix[...])
            square[...] = (
                mm(m_high[...], m_high[...])
                + mm(m_high[...], m_low[...])
                + mm(m_low[...], m_high[...])
            )
            q_high[...], q_low[...] = split(square[...])
            if repeat < ITERS - 1:
                cuts = ((slice(None), slice(None)),)
            else:
                cuts = tuple(
                    (slice(side * width, (side + 1) * width),) * 2 for side in range(2)
                )
            for across, down in cuts:
                cube = (
                    mm(q_high[across, :], m_high[:, down])
                    + mm(q_high[across, :], m_low[:, down])
                    + mm(q_low[across, :], m_high[:, down])
                )
                matrix[across, down] = 3.0 * square[across, down] - 2.0 * cube
        factor = jnp.where(live_ref[dimer] > 0, weights_ref[dimer], jnp.float32(0.0))
        for side in range(2):
            ref = 2 * dimer + side
            low = side * width
            mid = low + half
            high = low + width
            corner, mixed, diag_row = pack(
                factor * matrix[low:mid, low:mid],
                factor * matrix[low:mid, mid:high],
                factor * matrix[mid:high, mid:high],
            )

            def put_grown(piece, value, ref=ref):
                grown[piece, ref] = value

            scatter_rows(put_grown, corner, mixed)
            extra[ref:ref + 1, :] = diag_row
            extra[refs + ref:refs + ref + 1, :] = jnp.full((1, half), factor, F32)

    exchange(3, grown, landed, False)
    exchange(4, extra, landed_extra, True)
    landed[0] = grown[me]
    landed_extra[0] = extra[...]

    wait_for(recv_sems, 3, landed)
    if rows == 8:
        values = landed[...].reshape(lanes, half)
    else:
        for entry in range(count * refs):
            flat[entry * rows:(entry + 1) * rows, :] = landed[entry // refs, entry % refs]
        values = flat[...]
    first, rest = values.astype(BF16), None
    rest = values - first.astype(F32)
    second, third = split(rest)
    sums = mm(table[...], first) + mm(table[...], second) + mm(table[...], third)
    for piece in range(count):
        totals[piece] = sums[piece * rows:(piece + 1) * rows, :]
    exchange(5, totals, back, False)
    back[0] = totals[me]

    wait_for(recv_sems, 4, landed_extra)
    which = lax.broadcasted_iota(jnp.int32, (2 * refs, half), 0) % refs

    def collect(entry, carry):
        source = lax.rem(me + entry, count)
        mask = jnp.zeros((2 * refs, half), jnp.int32)
        for ref in range(refs):
            hit = jnp.where(refs_s[source * refs + ref] == me, 1, 0)
            mask = jnp.where(which == ref, hit, mask)
        return carry + jnp.where(mask > 0, landed_extra[entry], 0.0)

    side_sums = lax.fori_loop(
        0, count, collect, jnp.zeros((2 * refs, half), F32), unroll=count <= 32
    )
    diag_total = jnp.sum(side_sums[:refs], axis=0, keepdims=True)
    scale = 1.0 + jnp.sum(side_sums[refs:], axis=0, keepdims=True)

    wait_for(recv_sems, 5, back)
    for piece in range(count):
        joined[piece * rows:(piece + 1) * rows, :] = back[wrap(piece - me, count)]
    corner = joined[:half, :]
    mixed = joined[half:, :]
    turned = mixed.T
    out_ref[0, :half, :half] = (
        density_ref[0, :half, :half] + jnp.where(upper, mixed, turned)
    ) / scale
    out_ref[0, :half, half:] = (density_ref[0, :half, half:] + corner) / scale
    out_ref[0, half:, :half] = (density_ref[0, half:, :half] + corner.T) / scale
    out_ref[0, half:, half:] = (
        density_ref[0, half:, half:]
        + jnp.where(on_diag, diag_total, jnp.where(strict, mixed, turned))
    ) / scale

    for phase, target in enumerate((held, held_diag, got, landed, landed_extra, back)):
        wait_for(send_sems, phase, target)


def solution(mesh):
    count_x, count_y = mesh.shape["gx"], mesh.shape["gy"]
    count = count_x * count_y

    def per_device(density, coupling, weights, live_mask, dimer_pairs, dimer_slot, frag_slot):
        frag_dev, width, _ = density.shape
        dim_dev = coupling.shape[0]
        refs = 2 * dim_dev
        half = width // 2
        rows = width // count
        assert frag_dev == 1 and rows * count == width
        vmem = lambda *shape: pltpu.VMEM(shape, F32)
        bf16 = lambda *shape: pltpu.VMEM(shape, BF16)
        in_vmem = pl.BlockSpec(memory_space=pltpu.VMEM)
        in_smem = pl.BlockSpec(memory_space=pltpu.SMEM)
        return pl.pallas_call(
            functools.partial(kernel, count_x, count_y),
            out_shape=jax.ShapeDtypeStruct(density.shape, F32),
            in_specs=[in_vmem, in_vmem] + [in_smem] * 5,
            out_specs=in_vmem,
            scratch_shapes=[
                pltpu.SMEM((dimer_slot.shape[0],), jnp.int32),
                pltpu.SMEM((count * refs,), jnp.int32),
                vmem(count, rows, half),
                vmem(count, rows, half),
                vmem(1, half),
                vmem(count, 1, half),
                vmem(count, refs, rows, half),
                vmem(count, refs, rows, half),
                vmem(width, half),
                vmem(2 * width, 2 * width),
                bf16(2 * width, 2 * width),
                bf16(2 * width, 2 * width),
                bf16(2 * width, 2 * width),
                bf16(2 * width, 2 * width),
                vmem(2 * width, 2 * width),
                vmem(count, refs, rows, half),
                vmem(count, refs, rows, half),
                vmem(2 * refs, half),
                vmem(count, 2 * refs, half),
                vmem(count * refs * rows if rows != 8 else 8, half),
                bf16(count * rows, count * refs * rows),
                vmem(count, rows, half),
                vmem(count, rows, half),
                pltpu.SemaphoreType.DMA((6,)),
                pltpu.SemaphoreType.DMA((6,)),
            ],
            compiler_params=pltpu.CompilerParams(collective_id=0, has_side_effects=True),
        )(density, coupling, weights, live_mask, dimer_pairs, dimer_slot, frag_slot)

    both = ("gx", "gy")
    return jax.shard_map(
        per_device,
        mesh=mesh,
        in_specs=(
            P(both, None, None),
            P(both, None, None),
            P(both),
            P(both),
            P(),
            P(),
            P(),
        ),
        out_specs=P(both, None, None),
        check_vma=False,
    )
```

```python
import functools
import jax
import jax.numpy as jnp
from jax import lax
from jax.experimental import pallas as pl
from jax.experimental.pallas import tpu as pltpu
from jax.sharding import PartitionSpec as P

ITERS = 3
MESH = pl.DeviceIdType.MESH
F32 = jnp.float32
BF16 = jnp.bfloat16


def split(value):
    high = value.astype(BF16)
    return high, (value - high.astype(F32)).astype(BF16)


def mm(left, right):
    return jnp.dot(left, right, preferred_element_type=F32)


def wrap(index, count):
    return jnp.where(index < 0, index + count, index)


def grid_iota(rows, columns):
    return (
        lax.broadcasted_iota(jnp.int32, (rows, columns), 0),
        lax.broadcasted_iota(jnp.int32, (rows, columns), 1),
    )


def kernel(
    count_x, count_y,
    density_in, coupling_in, weights_in, live_in, pairs_in, dslot_in, fslot_in,
    out_ref,
    density_ref, coupling_ref, weights_ref, live_ref, pairs_ref, dslot_ref, fslot_ref,
    codes, refs_s, packed, held, diag, held_diag, chosen, got, joined,
    matrix, m_high, m_low, q_high, q_low, square,
    grown, landed, extra, landed_extra, flat, table, totals, back,
    send_sems, recv_sems, stage_sems,
):
    count = count_x * count_y
    dim_dev = coupling_ref.shape[0]
    refs = 2 * dim_dev
    dimers = dslot_ref.shape[0]
    width = density_ref.shape[1]
    half = width // 2
    rows = width // count
    me = lax.axis_index("gx") * count_y + lax.axis_index("gy")

    def peer(step):
        other = lax.rem(me + step, count)
        return other, (lax.div(other, count_y), lax.rem(other, count_y))

    barrier = pltpu.get_barrier_semaphore()

    def greet(step, carry):
        pl.semaphore_signal(barrier, inc=1, device_id=peer(step)[1], device_id_type=MESH)
        return carry

    lax.fori_loop(1, count, greet, 0)

    staged = [
        pltpu.make_async_copy(source, target, stage_sems.at[place])
        for place, (source, target) in enumerate((
            (density_in, density_ref), (dslot_in, dslot_ref), (fslot_in, fslot_ref),
            (pairs_in, pairs_ref), (weights_in, weights_ref), (live_in, live_ref),
            (coupling_in, coupling_ref),
        ))
    ]
    for copy in staged:
        copy.start()
    staged[0].wait()

    row_id, column_id = grid_iota(half, half)
    upper = row_id <= column_id
    strict = row_id > column_id
    on_diag = row_id == column_id

    def pack(first, corner, second):
        mixed = jnp.where(upper, first, second)
        return corner, mixed, jnp.sum(jnp.where(on_diag, second, 0.0), axis=0, keepdims=True)

    def scatter_rows(target, corner, mixed):
        for piece in range(count):
            start = piece * rows
            source = corner if start < half else mixed
            start = start % half
            target(piece, source[start:start + rows])

    corner, mixed, diag_row = pack(
        density_ref[0, :half, :half], density_ref[0, :half, half:], density_ref[0, half:, half:]
    )

    def put_packed(piece, value):
        packed[piece] = value

    scatter_rows(put_packed, corner, mixed)
    diag[...] = diag_row

    pl.semaphore_wait(barrier, count - 1)

    def exchange(phase, source, target, same):
        def send(turn, carry, lag):
            step = turn * count_y + lag
            other, where_to = peer(step)
            pltpu.make_async_remote_copy(
                src_ref=source if same else source.at[other],
                dst_ref=target.at[count - step],
                send_sem=send_sems.at[phase],
                recv_sem=recv_sems.at[phase],
                device_id=where_to,
                device_id_type=MESH,
            ).start()
            return carry

        for lag in sorted(range(count_y), key=lambda lag: -min(lag, count_y - lag)):
            lax.fori_loop(
                0 if lag else 1, count_x, functools.partial(send, lag=lag), 0, unroll=count_x <= 8
            )

    def wait_for(sems, phase, target):
        span = target.at[pl.ds(1, count - 1)]
        pltpu.make_async_copy(span, span, sems.at[phase]).wait()

    exchange(0, packed, held, False)
    exchange(1, diag, held_diag, True)
    held[0] = packed[me]
    held_diag[0] = diag[...]

    for copy in staged[1:]:
        copy.wait()

    def code_of(dimer, carry):
        codes[dimer] = fslot_ref[pairs_ref[0, dimer]] * count + fslot_ref[pairs_ref[1, dimer]]
        return carry

    lax.fori_loop(0, dimers, code_of, 0)

    def names(slot, carry):
        def look(dimer, found):
            return jnp.where(dslot_ref[dimer] == slot, codes[dimer], found)

        found = lax.fori_loop(0, dimers, look, jnp.int32(0), unroll=dimers <= 64)
        refs_s[2 * slot] = lax.div(found, jnp.int32(count))
        refs_s[2 * slot + 1] = lax.rem(found, jnp.int32(count))
        return carry

    lax.fori_loop(0, count * dim_dev, names, 0)

    wait_for(recv_sems, 0, held)

    def choose(target, carry):
        for ref in range(refs):
            slot = refs_s[target * refs + ref]
            chosen[target, ref] = held[wrap(slot - me, count)]
        return carry

    lax.fori_loop(0, count, choose, 0, unroll=count <= 32)
    exchange(2, chosen, got, False)
    got[0] = chosen[me]
    wait_for(recv_sems, 1, held_diag)

    lanes = count * refs * rows
    lane_id = lax.broadcasted_iota(jnp.int32, (1, lanes), 1)
    lane_ref = lane_id // rows

    def spread(entry, row):
        ref = lax.rem(entry, refs)
        source = lax.rem(me + lax.div(entry, refs), count)
        return jnp.where(lane_ref == entry, refs_s[source * refs + ref], row)

    named = lax.fori_loop(
        0, count * refs, spread, jnp.zeros((1, lanes), jnp.int32), unroll=count * refs <= 64
    )
    named = named * rows + lane_id % rows
    table_row = lax.broadcasted_iota(jnp.int32, (count * rows, lanes), 0)
    table[...] = jnp.where(table_row == named, 1.0, 0.0).astype(BF16)

    def couple(dimer):
        coupled = coupling_ref[dimer]
        matrix[:width, width:] = coupled
        matrix[width:, :width] = coupled.T

    couple(0)
    wait_for(recv_sems, 2, got)

    for dimer in range(dim_dev):
        if dimer:
            couple(dimer)
        for side in range(2):
            ref = 2 * dimer + side
            for piece in range(count):
                joined[piece * rows:(piece + 1) * rows, :] = got[wrap(piece - me, count), ref]
            corner = joined[:half, :]
            mixed = joined[half:, :]
            turned = mixed.T
            slot = refs_s[me * refs + ref]
            diag_row = held_diag[wrap(slot - me, count)]
            low = side * width
            mid = low + half
            high = low + width
            matrix[low:mid, low:mid] = jnp.where(upper, mixed, turned)
            matrix[low:mid, mid:high] = corner
            matrix[mid:high, low:mid] = corner.T
            matrix[mid:high, mid:high] = jnp.where(
                on_diag, diag_row, jnp.where(strict, mixed, turned)
            )
        for repeat in range(ITERS):
            m_high[...], m_low[...] = split(matrix[...])
            square[...] = (
                mm(m_high[...], m_high[...])
                + mm(m_high[...], m_low[...])
                + mm(m_low[...], m_high[...])
            )
            q_high[...], q_low[...] = split(square[...])
            if repeat < ITERS - 1:
                cuts = ((slice(None), slice(None)),)
            else:
                cuts = tuple(
                    (slice(side * width, (side + 1) * width),) * 2 for side in range(2)
                )
            for across, down in cuts:
                cube = (
                    mm(q_high[across, :], m_high[:, down])
                    + mm(q_high[across, :], m_low[:, down])
                    + mm(q_low[across, :], m_high[:, down])
                )
                matrix[across, down] = 3.0 * square[across, down] - 2.0 * cube
        factor = jnp.where(live_ref[dimer] > 0, weights_ref[dimer], jnp.float32(0.0))
        for side in range(2):
            ref = 2 * dimer + side
            low = side * width
            mid = low + half
            high = low + width
            corner, mixed, diag_row = pack(
                factor * matrix[low:mid, low:mid],
                factor * matrix[low:mid, mid:high],
                factor * matrix[mid:high, mid:high],
            )

            def put_grown(piece, value, ref=ref):
                grown[piece, ref] = value

            scatter_rows(put_grown, corner, mixed)
            extra[ref:ref + 1, :] = diag_row
            extra[refs + ref:refs + ref + 1, :] = jnp.full((1, half), factor, F32)

    exchange(3, grown, landed, False)
    exchange(4, extra, landed_extra, True)
    landed[0] = grown[me]
    landed_extra[0] = extra[...]

    wait_for(recv_sems, 3, landed)
    if rows == 8:
        values = landed[...].reshape(lanes, half)
    else:
        for entry in range(count * refs):
            flat[entry * rows:(entry + 1) * rows, :] = landed[entry // refs, entry % refs]
        values = flat[...]
    first, rest = values.astype(BF16), None
    rest = values - first.astype(F32)
    second, third = split(rest)
    sums = mm(table[...], first) + mm(table[...], second) + mm(table[...], third)
    for piece in range(count):
        totals[piece] = sums[piece * rows:(piece + 1) * rows, :]
    exchange(5, totals, back, False)
    back[0] = totals[me]

    wait_for(recv_sems, 4, landed_extra)
    which = lax.broadcasted_iota(jnp.int32, (2 * refs, half), 0) % refs

    def collect(entry, carry):
        source = lax.rem(me + entry, count)
        mask = jnp.zeros((2 * refs, half), jnp.int32)
        for ref in range(refs):
            hit = jnp.where(refs_s[source * refs + ref] == me, 1, 0)
            mask = jnp.where(which == ref, hit, mask)
        return carry + jnp.where(mask > 0, landed_extra[entry], 0.0)

    side_sums = lax.fori_loop(
        0, count, collect, jnp.zeros((2 * refs, half), F32), unroll=count <= 32
    )
    diag_total = jnp.sum(side_sums[:refs], axis=0, keepdims=True)
    scale = 1.0 + jnp.sum(side_sums[refs:], axis=0, keepdims=True)

    wait_for(recv_sems, 5, back)
    for piece in range(count):
        joined[piece * rows:(piece + 1) * rows, :] = back[wrap(piece - me, count)]
    corner = joined[:half, :]
    mixed = joined[half:, :]
    turned = mixed.T
    out_ref[0, :half, :half] = (
        density_ref[0, :half, :half] + jnp.where(upper, mixed, turned)
    ) / scale
    out_ref[0, :half, half:] = (density_ref[0, :half, half:] + corner) / scale
    out_ref[0, half:, :half] = (density_ref[0, half:, :half] + corner.T) / scale
    out_ref[0, half:, half:] = (
        density_ref[0, half:, half:]
        + jnp.where(on_diag, diag_total, jnp.where(strict, mixed, turned))
    ) / scale

    for phase, target in enumerate((held, held_diag, got, landed, landed_extra, back)):
        wait_for(send_sems, phase, target)


def solution(mesh):
    count_x, count_y = mesh.shape["gx"], mesh.shape["gy"]
    count = count_x * count_y

    def per_device(density, coupling, weights, live_mask, dimer_pairs, dimer_slot, frag_slot):
        frag_dev, width, _ = density.shape
        dim_dev = coupling.shape[0]
        refs = 2 * dim_dev
        half = width // 2
        rows = width // count
        assert frag_dev == 1 and rows * count == width
        vmem = lambda *shape: pltpu.VMEM(shape, F32)
        bf16 = lambda *shape: pltpu.VMEM(shape, BF16)
        in_vmem = pl.BlockSpec(memory_space=pltpu.VMEM)
        smem = lambda array: pltpu.SMEM(array.shape, array.dtype)
        pairs = dimer_pairs.T
        return pl.pallas_call(
            functools.partial(kernel, count_x, count_y),
            out_shape=pltpu.VMEM(density.shape, F32),
            in_specs=[pl.BlockSpec(memory_space=pl.ANY)] * 7,
            out_specs=in_vmem,
            scratch_shapes=[
                vmem(*density.shape),
                vmem(*coupling.shape),
                smem(weights),
                smem(live_mask),
                smem(pairs),
                smem(dimer_slot),
                smem(frag_slot),
                pltpu.SMEM((dimer_slot.shape[0],), jnp.int32),
                pltpu.SMEM((count * refs,), jnp.int32),
                vmem(count, rows, half),
                vmem(count, rows, half),
                vmem(1, half),
                vmem(count, 1, half),
                vmem(count, refs, rows, half),
                vmem(count, refs, rows, half),
                vmem(width, half),
                vmem(2 * width, 2 * width),
                bf16(2 * width, 2 * width),
                bf16(2 * width, 2 * width),
                bf16(2 * width, 2 * width),
                bf16(2 * width, 2 * width),
                vmem(2 * width, 2 * width),
                vmem(count, refs, rows, half),
                vmem(count, refs, rows, half),
                vmem(2 * refs, half),
                vmem(count, 2 * refs, half),
                vmem(count * refs * rows if rows != 8 else 8, half),
                bf16(count * rows, count * refs * rows),
                vmem(count, rows, half),
                vmem(count, rows, half),
                pltpu.SemaphoreType.DMA((6,)),
                pltpu.SemaphoreType.DMA((6,)),
                pltpu.SemaphoreType.DMA((7,)),
            ],
            compiler_params=pltpu.CompilerParams(collective_id=0, has_side_effects=True),
        )(density, coupling, weights, live_mask, pairs, dimer_slot, frag_slot)

    both = ("gx", "gy")
    return jax.shard_map(
        per_device,
        mesh=mesh,
        in_specs=(
            P(both, None, None),
            P(both, None, None),
            P(both),
            P(both),
            P(),
            P(),
            P(),
        ),
        out_specs=P(both, None, None),
        check_vma=False,
    )
```
